128 devices in a mesh: gx: 8 (over y, core), gy: 16 (over z, x).
Axes of the slice: x: 4, y: 4, z: 4, core: 2. Of those that a mesh axis runs over, the one named last changes fastest.
Arguments:
- a_rows: bfloat16 [786432, 1024], P(('gx', 'gy')), may hold values from -24 to 24
- heights: int32 [128], P('gx'), may hold values from 1 to 44, as said below
- destination: int32 [128, 48], P('gx'), may hold values from 0 to 4095, as said below
Outputs:
- ortho_rows: bfloat16 [524288, 1024], P(('gx', 'gy'))
- factor_r: float32 [1024, 1024], replicated
The draws below stay inside these ranges and needn't reach their ends.
Inputs may be any that keep to these rules, and one draw needn't show every extreme that they name: Tiles 0 to heights[d] - 1 of device d are live, the others carry nothing of the problem; the largest value is reached in every draw. For a live tile, destination // 32 is a device with the same gx index as the tile's device; live tiles name distinct slots; one device sends at most one live tile to any other device; entries of tiles that are not live are meaningless.
All inputs are finite; a program needn't handle non-finite values.
Results may differ from the reference program's by a relative error of at most 0.00055.
Values may be sent and summed in bfloat16 or wider, within the bound.
No kernel may reach another device: no remote copies, remote signals or barrier semaphores. Data moves between devices by JAX's collectives and lax.ppermute only.
A program may use at most 256 MiB of HBM per device.

```python
import math
import jax
import jax.numpy as jnp
from jax import lax

W = 1024
TILE = 128
SLOTS = 32
TILES = 48
N_GY = 16
DEVICES = 128


def plan_tiles(key):
    base = jax.random.fold_in(key, 7)
    keys = jax.random.split(base, 6)
    group_size = N_GY
    groups = DEVICES // group_size
    heavy_count = group_size // 4
    light_count = group_size - heavy_count
    extra = min(TILES - SLOTS, light_count)
    ordering = jax.vmap(lambda sub: jax.random.permutation(sub, group_size))(jax.random.split(keys[0], groups)).astype(jnp.int32)
    ranking = jnp.argsort(ordering, axis=1).astype(jnp.int32)
    heavy = ranking < heavy_count
    high = jax.random.randint(keys[1], (groups, group_size), SLOTS + 1, SLOTS + extra + 1)
    high = jnp.where(ranking == 0, SLOTS + extra, high)
    small = jax.random.randint(keys[2], (groups, group_size), 1, SLOTS - heavy_count + 1)
    height = jnp.where(heavy, high, small).astype(jnp.int32)
    excess_rank = jnp.take_along_axis(height, ordering, 1) - SLOTS
    flat_height = height.reshape(-1)
    tile_perm = jax.vmap(lambda sub: jax.random.permutation(sub, TILES))(jax.random.split(keys[3], DEVICES)).astype(jnp.int32)
    tile_ids = jnp.arange(TILES, dtype=jnp.int32)
    tile_live = tile_ids[None, :] < flat_height[:, None]
    tile_order = jnp.argsort(jnp.where(tile_live, tile_perm, tile_perm + TILES), axis=1).astype(jnp.int32)
    position = jnp.argsort(tile_order, axis=1).astype(jnp.int32)
    kept = jnp.minimum(flat_height, SLOTS)
    rank_flat = ranking.reshape(-1)
    offset = position - kept[:, None]
    leaving = tile_live & (offset >= 0)
    light_target = jnp.mod(rank_flat[:, None] + offset, light_count)
    group_ids = jnp.arange(DEVICES, dtype=jnp.int32) // group_size
    target_gy = jnp.take_along_axis(ordering[group_ids], heavy_count + light_target, 1)
    device_ids = jnp.arange(DEVICES, dtype=jnp.int32)
    target_dev = jnp.where(leaving, group_ids[:, None] * group_size + target_gy, device_ids[:, None])
    heavy_ids = jnp.arange(heavy_count, dtype=jnp.int32)
    light_ids = jnp.arange(light_count, dtype=jnp.int32)
    sends = jnp.mod(light_ids[None, :] - heavy_ids[:, None], light_count)[None] < excess_rank[:, :heavy_count, None]
    sends_int = sends.astype(jnp.int32)
    before = jnp.cumsum(sends_int, axis=1) - sends_int
    slot_perm = jax.vmap(lambda sub: jax.random.permutation(sub, SLOTS))(jax.random.split(keys[4], DEVICES)).astype(jnp.int32)
    kept_slot = jnp.take_along_axis(slot_perm, jnp.minimum(position, SLOTS - 1), 1)
    sender_rank = jnp.broadcast_to(jnp.minimum(rank_flat, heavy_count - 1)[:, None], (DEVICES, TILES))
    group_grid = jnp.broadcast_to(group_ids[:, None], (DEVICES, TILES))
    recv_rank = before[group_grid, sender_rank, light_target]
    recv_kept = kept[target_dev]
    sent_slot = slot_perm[target_dev, jnp.minimum(recv_kept + recv_rank, SLOTS - 1)]
    chosen_slot = jnp.where(leaving, sent_slot, kept_slot)
    filler = jax.random.randint(keys[5], (DEVICES, TILES), 0, DEVICES * SLOTS)
    mapped = jnp.where(tile_live, target_dev * SLOTS + chosen_slot, filler)
    return (flat_height.astype(jnp.int32), mapped.astype(jnp.int32))


def draw_heights(key, part):
    return plan_tiles(key)[0]


def draw_destination(key, part):
    return plan_tiles(key)[1]


def raised(array, stream_key, source, target, blocks, factor):
    def block_of(dim):
        return (jnp.arange(array.shape[dim]) // (array.shape[dim] // blocks)).reshape((-1,) + (1,) * (array.ndim - 1 - dim))

    near = jax.random.permutation(stream_key, blocks)[block_of(target)]
    far = (block_of(target) + blocks // 2) % blocks
    return jnp.where((block_of(source) == near) | (block_of(source) == far), factor * array, array)


def shard_levels(own_key, extent, cuts, smallest, top_value):
    def one(dim, parts):
        steps = jax.random.uniform(jax.random.fold_in(jax.random.fold_in(own_key, 6), dim), (parts,), jnp.float32, smallest / len(cuts), top_value / len(cuts))
        return jnp.repeat(jnp.exp(steps), extent[dim] // parts).reshape((-1,) + (1,) * (len(extent) - dim - 1))

    gain = one(*cuts[0])
    for cut in cuts[1:]:
        gain = gain * one(*cut)
    return gain


def bell_draw_with(stream_key, dims, scale, reach, shards, heavy, kind=jnp.bfloat16):
    result = scale * jax.random.normal(stream_key, dims, jnp.float32)
    if shards:
        result = result * shard_levels(stream_key, dims, shards, -0.22, 0.18)
    return jnp.clip(raised(result, jax.random.fold_in(stream_key, 3), *heavy), -reach, reach).astype(kind)


def setup_inputs(seed: int = 0) -> dict:
    seeds = jax.random.split(jax.random.key(seed), 4)
    a_rows = bell_draw_with(seeds[0], (DEVICES * TILES * TILE, W), 1.0, 24.0, ((0, 128),), (0, 1, 128, 5.5))
    heights = draw_heights(jax.random.fold_in(seeds[3], 71), 0)
    destination = draw_destination(jax.random.fold_in(seeds[3], 71), 0)
    return dict(a_rows=a_rows, heights=heights, destination=destination)


def reference(a_rows, heights, destination):
    dev_count = heights.shape[0]
    tile_stack = a_rows.reshape(dev_count * TILES, TILE, W)
    tile_live = (jnp.arange(TILES, dtype=jnp.int32)[None, :] < heights[:, None]).reshape(-1)
    target = jnp.where(tile_live, destination.reshape(-1), dev_count * SLOTS).astype(jnp.int32)
    balanced = jnp.zeros((dev_count * SLOTS, TILE, W), jnp.bfloat16).at[target].set(tile_stack, mode='drop')
    slabs = balanced.reshape(dev_count, SLOTS * TILE, W)

    def accumulate(running, slab_rows):
        product = lax.dot_general(slab_rows.astype(jnp.float32), slab_rows.astype(jnp.float32), (((0,), (0,)), ((), ())), preferred_element_type=jnp.float32)
        return (running + product, None)
    gram, _ = lax.scan(accumulate, jnp.zeros((W, W), jnp.float32), slabs)
    low_factor = jnp.linalg.cholesky(gram)
    root_scale = math.sqrt(dev_count * SLOTS * TILE)

    def orthonormal(slab_rows):
        solved = jax.scipy.linalg.solve_triangular(low_factor, slab_rows.astype(jnp.float32).T, lower=True)
        return (solved.T * root_scale).astype(jnp.bfloat16)
    ortho_rows = lax.map(orthonormal, slabs).reshape(-1, W)
    return (ortho_rows, low_factor.T / root_scale)
```

```python
import math

import jax
import jax.numpy as jnp
from jax import lax
from jax.experimental import pallas as pl
from jax.experimental.pallas import tpu as pltpu
from jax.sharding import Mesh, PartitionSpec as P

TILE = 128
SLOTS = 32
W = 1024
NB = W // 128
MAX_LIVE = 44
CHUNK = 4
GROUP = 4
F32 = jnp.float32
BF16 = jnp.bfloat16
BLOCKS = [(i, j) for i in range(NB) for j in range(i, NB)]
HALF = len(BLOCKS) // 2
CHIPS = ("y", "z", "x")


def gram_kernel(heights_ref, x_ref, mine_ref, other_ref, acc_ref):
    step = pl.program_id(0)
    pos = lax.axis_index("z") * lax.axis_size("x") + lax.axis_index("x")
    core = lax.axis_index("core")
    live = heights_ref[pos]

    @pl.when(step == 0)
    def _():
        acc_ref[...] = jnp.zeros_like(acc_ref)

    def accumulate(x):
        for i in range(0, W, 256):
            acc_ref[i : i + 256, i:] += lax.dot_general(
                x[:, i : i + 256], x[:, i:], (((0,), (0,)), ((), ())), preferred_element_type=F32
            )

    @pl.when((step + 1) * CHUNK <= live)
    def _():
        accumulate(x_ref[...])

    @pl.when((step * CHUNK < live) & ((step + 1) * CHUNK > live))
    def _():
        rows = lax.broadcasted_iota(jnp.int32, x_ref.shape, 0)
        kept = rows < (live - step * CHUNK) * TILE
        accumulate(jnp.where(kept, x_ref[...].astype(F32), 0.0).astype(BF16))

    def put(ref, blocks):
        for b, (i, j) in enumerate(blocks):
            ref[b] = acc_ref[i * 128 : i * 128 + 128, j * 128 : j * 128 + 128]

    last = step == pl.num_programs(0) - 1

    @pl.when(last & (core == 0))
    def _():
        put(mine_ref, BLOCKS[:HALF])
        put(other_ref, BLOCKS[HALF:])

    @pl.when(last & (core == 1))
    def _():
        put(mine_ref, BLOCKS[HALF:])
        put(other_ref, BLOCKS[:HALF])


def gram(a_rows, heights):
    steps = -(-MAX_LIVE // CHUNK)

    def chunk_map(step, heights_ref):
        pos = lax.axis_index("z") * lax.axis_size("x") + lax.axis_index("x")
        return (jnp.minimum(step, lax.div(heights_ref[pos] + (CHUNK - 1), CHUNK) - 1), 0)

    whole = pl.BlockSpec((HALF, 128, 128), lambda step, heights_ref: (0, 0, 0))
    return pl.pallas_call(
        gram_kernel,
        grid_spec=pltpu.PrefetchScalarGridSpec(
            num_scalar_prefetch=1,
            grid=(steps,),
            in_specs=[pl.BlockSpec((CHUNK * TILE, W), chunk_map)],
            out_specs=[whole, whole],
            scratch_shapes=[pltpu.VMEM((W, W), F32)],
        ),
        out_shape=[jax.ShapeDtypeStruct((HALF, 128, 128), F32)] * 2,
        name="gram",
    )(heights, a_rows)


def pick_kernel(index_ref, a_ref, out_ref, buf_ref, in_sems, out_sems):
    count = out_ref.shape[0]
    loads = [
        pltpu.make_async_copy(a_ref.at[pl.ds(pl.multiple_of(index_ref[i] * TILE, TILE), TILE)], buf_ref.at[i], in_sems.at[i])
        for i in range(count)
    ]
    stores = [pltpu.make_async_copy(buf_ref.at[i], out_ref.at[i], out_sems.at[i]) for i in range(count)]
    for load in loads:
        load.start()
    for load, store in zip(loads, stores):
        load.wait()
        store.start()
    for store in stores:
        store.wait()


def pick_tiles(a_rows, index):
    count = index.shape[0]
    return pl.pallas_call(
        pick_kernel,
        grid_spec=pltpu.PrefetchScalarGridSpec(
            num_scalar_prefetch=1,
            grid=(),
            in_specs=[pl.BlockSpec(memory_space=pl.ANY)],
            out_specs=pl.BlockSpec(memory_space=pl.ANY),
            scratch_shapes=[
                pltpu.VMEM((count, TILE, W), BF16),
                pltpu.SemaphoreType.DMA((count,)),
                pltpu.SemaphoreType.DMA((count,)),
            ],
        ),
        out_shape=jax.ShapeDtypeStruct((count, TILE, W), BF16),
        name="pick",
    )(index, a_rows)


def lane_bcast(v, lane):
    return jnp.broadcast_to(v[:, lane : lane + 1], (8, 128))


def row_bcast(ref, p, s):
    return jnp.broadcast_to(ref[p, s : s + 1, :], (8, 128))


def factor_block(d_ref, rk_ref, dk_ref, es_ref, vs_ref, ws_ref):
    sub = lax.broadcasted_iota(jnp.int32, (8, 128), 0)
    lane = lax.broadcasted_iota(jnp.int32, (8, 128), 1)
    v = [d_ref[8 * g : 8 * g + 8, :] for g in range(16)]
    w = [jnp.where(lane == sub + 8 * g, 1.0, 0.0).astype(F32) for g in range(16)]

    def entries(q):
        for j in range(8):
            es_ref[8 * q + j] = lane_bcast(v[q], 8 * q + j)
        return {(i, j): row_bcast(es_ref, 8 * q + j, i) for j in range(8) for i in range(j, 8)}

    e = entries(0)
    for p in range(16):
        vs_ref[p] = v[p]
        ws_ref[p] = w[p]
        low, inv, rows, wide = {}, [], [], []
        for s in range(8):
            inv.append(lax.rsqrt(e[s, s]))
            for i in range(s + 1, 8):
                low[i, s] = e[i, s] * inv[s]
            for j in range(s + 1, 8):
                for i in range(j, 8):
                    e[i, j] = e[i, j] - low[i, s] * low[j, s]
            r, q = row_bcast(vs_ref, p, s), row_bcast(ws_ref, p, s)
            for t in range(s):
                r = r - low[s, t] * rows[t]
                q = q - low[s, t] * wide[t]
            rows.append(r * inv[s])
            wide.append(q * inv[s])
        for s in range(8):
            rk_ref[8 * p + s : 8 * p + s + 1, :] = rows[s][0:1]
            dk_ref[8 * p + s : 8 * p + s + 1, :] = wide[s][0:1]
        if p == 15:
            break
        e = entries(p + 1)
        spread = [[lane_bcast(rows[s], 8 * p + 8 + i) for i in range(8)] for s in range(8)]
        for s in range(8):
            for j in range(8):
                for i in range(j, 8):
                    e[i, j] = e[i, j] - spread[s][i] * spread[s][j]
        for g in range(p + 1, 16):
            for s in range(8):
                m = jnp.take_along_axis(rows[s], sub + 8 * g, axis=1, mode="promise_in_bounds")
                v[g] = v[g] - m * rows[s]
                w[g] = w[g] - m * wide[s]


def split3(x):
    h = x.astype(BF16)
    r = x - h.astype(F32)
    m = r.astype(BF16)
    return h, m, (r - m.astype(F32)).astype(BF16)


def put_left(ref, x):
    h, m, l = split3(x)
    ref[:, 0:128] = l
    ref[:, 128:256] = h
    ref[:, 256:384] = m
    ref[:, 384:512] = h


def put_right(ref, x):
    h, m, l = split3(x)
    ref[0:128] = m
    ref[128:256] = h
    ref[256:384] = l


def product(left_ref, right_ref):
    dot = lambda a, b: jnp.dot(a, b, preferred_element_type=F32)
    return (
        dot(left_ref[:, 0:256], right_ref[128:384])
        + dot(left_ref[:, 128:384], right_ref[0:256])
        + dot(left_ref[:, 256:512], right_ref[0:256])
    )


def chol_kernel(root, mine_ref, other_ref, hi_ref, lo_ref, r_ref, t_ref, d_ref, rk_ref, dk_ref, p_ref, left_ref, right_ref, es_ref, vs_ref, ws_ref):
    core = lax.axis_index("core")

    def take(ref, blocks):
        for b, (i, j) in enumerate(blocks):
            t_ref[i * 128 : i * 128 + 128, j * 128 : j * 128 + 128] = ref[b]

    @pl.when(core == 0)
    def _():
        take(mine_ref, BLOCKS[:HALF])
        take(other_ref, BLOCKS[HALF:])

    @pl.when(core == 1)
    def _():
        take(mine_ref, BLOCKS[HALF:])
        take(other_ref, BLOCKS[:HALF])

    sub = lax.broadcasted_iota(jnp.int32, (128, 128), 0)
    lane = lax.broadcasted_iota(jnp.int32, (128, 128), 1)
    wide_lane = lax.broadcasted_iota(jnp.int32, (128, W), 1)

    def block_row(k, carry):
        at = pl.multiple_of(k * 128, 128)
        here = pl.ds(at, 128)
        d_ref[...] = t_ref[here, here]
        factor_block(d_ref, rk_ref, dk_ref, es_ref, vs_ref, ws_ref)
        put_left(left_ref, dk_ref[...])
        put_right(right_ref, t_ref[here, :])
        p_ref[...] = product(left_ref, right_ref)
        r_ref[here, :] = jnp.where(wide_lane >= at + 128, p_ref[...] * (1.0 / root), 0.0)
        r_ref[here, here] = jnp.where(lane >= sub, rk_ref[...] * (1.0 / root), 0.0)
        p_ref[:, here] = dk_ref[...]
        scaled = jnp.where(wide_lane < at + 128, p_ref[...] * root, 0.0)
        hi = scaled.astype(BF16)
        hi_ref[here, :] = hi
        lo_ref[here, :] = (scaled - hi.astype(F32)).astype(BF16)
        put_right(right_ref, p_ref[...])

        def trailing(i, carry):
            below = pl.ds(pl.multiple_of(i * 128, 128), 128)
            put_left(left_ref, p_ref[:, below].T)
            t_ref[below, here] = jnp.zeros((128, 128), F32)
            t_ref[below, :] -= product(left_ref, right_ref)
            return carry

        lax.fori_loop(k + 1, NB, trailing, 0)
        return carry

    lax.fori_loop(0, NB, block_row, 0)


def cholesky(mine, other, root):
    return pl.pallas_call(
        lambda *refs: chol_kernel(root, *refs),
        out_shape=[
            jax.ShapeDtypeStruct((W, W), BF16),
            jax.ShapeDtypeStruct((W, W), BF16),
            jax.ShapeDtypeStruct((W, W), F32),
        ],
        scratch_shapes=[
            pltpu.VMEM((W, W), F32),
            pltpu.VMEM((128, 128), F32),
            pltpu.VMEM((128, 128), F32),
            pltpu.VMEM((128, 128), F32),
            pltpu.VMEM((128, W), F32),
            pltpu.VMEM((128, 512), BF16),
            pltpu.VMEM((384, W), BF16),
            pltpu.VMEM((128, 8, 128), F32),
            pltpu.VMEM((16, 8, 128), F32),
            pltpu.VMEM((16, 8, 128), F32),
        ],
        cost_estimate=pl.CostEstimate(flops=40_000_000_000, bytes_accessed=16_000_000, transcendentals=0),
        name="factor",
    )(mine, other)


def ortho_kernel(source_ref, filled_ref, a_ref, in_ref, hi_ref, lo_ref, out_ref, buf_ref, sems):
    step = pl.program_id(0)
    stored = a_ref.shape[0] // TILE

    def fetch(at, slot):
        for g in range(GROUP):
            src = source_ref[at * GROUP + g]
            dst = buf_ref.at[slot, pl.ds(g * TILE, TILE)]

            @pl.when(src < stored)
            def _():
                row = pl.multiple_of(src * TILE, TILE)
                pltpu.make_async_copy(a_ref.at[pl.ds(row, TILE)], dst, sems.at[slot, g]).start()

            @pl.when(src >= stored)
            def _():
                pltpu.make_async_copy(in_ref.at[src - stored], dst, sems.at[slot, g]).start()

    slot = lax.rem(step, 2)

    @pl.when(step == 0)
    def _():
        fetch(0, 0)

    @pl.when(step + 1 < pl.num_programs(0))
    def _():
        fetch(step + 1, 1 - slot)

    for g in range(GROUP):
        here = buf_ref.at[slot, pl.ds(g * TILE, TILE)]
        pltpu.make_async_copy(a_ref.at[pl.ds(0, TILE)], here, sems.at[slot, g]).wait()

        @pl.when(filled_ref[step * GROUP + g] == 0)
        def _():
            here[...] = jnp.zeros((TILE, W), BF16)

    nt = (((1,), (1,)), ((), ()))
    for j in range(0, W, 256):
        x = buf_ref[slot, :, : j + 256]
        acc = lax.dot_general(x, hi_ref[j : j + 256, : j + 256], nt, preferred_element_type=F32)
        acc += lax.dot_general(x, lo_ref[j : j + 256, : j + 256], nt, preferred_element_type=F32)
        out_ref[:, j : j + 256] = acc.astype(BF16)


def ortho(a_rows, received, source, filled, hi, lo):
    rows = GROUP * TILE
    square = pl.BlockSpec((W, W), lambda step, *_: (0, 0))
    return pl.pallas_call(
        ortho_kernel,
        grid_spec=pltpu.PrefetchScalarGridSpec(
            num_scalar_prefetch=2,
            grid=(SLOTS // GROUP,),
            in_specs=[pl.BlockSpec(memory_space=pl.ANY), pl.BlockSpec(memory_space=pl.ANY), square, square],
            out_specs=pl.BlockSpec((rows, W), lambda step, *_: (step, 0)),
            scratch_shapes=[pltpu.VMEM((2, rows, W), BF16), pltpu.SemaphoreType.DMA((2, GROUP))],
        ),
        out_shape=jax.ShapeDtypeStruct((SLOTS * TILE, W), BF16),
        name="ortho",
    )(source, filled, a_rows, received, hi, lo)


def plan(heights, destination):
    size_gy = lax.axis_size("z") * lax.axis_size("x")
    group_pos = lax.axis_index("z") * lax.axis_size("x") + lax.axis_index("x")
    group_base = (lax.axis_index("y") * lax.axis_size("core") + lax.axis_index("core")) * size_gy
    my_index = group_base + group_pos
    stored = destination.shape[1]
    tile_ids = jnp.arange(stored, dtype=jnp.int32)
    peer_ids = jnp.arange(size_gy, dtype=jnp.int32)
    slot_ids = jnp.arange(SLOTS, dtype=jnp.int32)
    tile_live = tile_ids[None, :] < heights[:, None]
    target_dev = destination // SLOTS
    target_slot = destination % SLOTS
    own_live = tile_live[group_pos]
    own_dev = target_dev[group_pos]
    own_slot = target_slot[group_pos]
    leaving = own_live & (own_dev != my_index)
    chosen = leaving[None, :] & (own_dev[None, :] - group_base == peer_ids[:, None])
    send_index = jnp.sum(jnp.where(chosen, tile_ids[None, :], 0), axis=1)
    arriving = tile_live & (target_dev == my_index) & (peer_ids[:, None] != group_pos)
    arrive_slot = jnp.sum(jnp.where(arriving, target_slot, 0), axis=1)
    arrive_has = jnp.any(arriving, axis=1)
    staying = own_live & (own_dev == my_index)
    own_match = staying[None, :] & (own_slot[None, :] == slot_ids[:, None])
    in_match = arrive_has[None, :] & (arrive_slot[None, :] == slot_ids[:, None])
    matched = jnp.concatenate([own_match, in_match], axis=1)
    places = jnp.arange(stored + size_gy, dtype=jnp.int32)
    source = jnp.sum(jnp.where(matched, places[None, :], 0), axis=1)
    filled = jnp.any(matched, axis=1).astype(jnp.int32)
    return send_index, source, filled


def swap_core(x):
    return lax.ppermute(x, "core", [(0, 1), (1, 0)])


def exchange(x, axes):
    return lax.all_to_all(x, axes, split_axis=0, concat_axis=0, tiled=True)


def on_device(a_rows, heights, destination):
    chips = math.prod(lax.axis_size(name) for name in CHIPS)
    root = math.sqrt(chips * 2 * SLOTS * TILE)
    mine, other = gram(a_rows, heights)
    half = (mine + swap_core(other)).reshape(chips, -1, 128)
    shard = jnp.sum(exchange(half, CHIPS), axis=0)
    send_index, source, filled = plan(heights, destination)
    tiles = pick_tiles(a_rows, send_index)
    full = exchange(jnp.broadcast_to(shard[None], half.shape), CHIPS)
    tiles, full = lax.optimization_barrier((tiles, full))
    mine = full.reshape(HALF, 128, 128)
    other = swap_core(mine)
    received = exchange(tiles, ("z", "x"))
    hi, lo, factor_r = cholesky(mine, other, root)
    ortho_rows = ortho(a_rows, received, source, filled, hi, lo)
    return (ortho_rows, factor_r)


def solution(mesh):
    fine = Mesh(mesh.devices.reshape(4, 2, 4, 4), ("y", "core", "z", "x"))
    every = ("y", "core", "z", "x")
    return jax.shard_map(
        on_device,
        mesh=fine,
        in_specs=(P(every, None), P(("y", "core")), P(("y", "core"), None)),
        out_specs=(P(every, None), P()),
        check_vma=False,
    )
```

```python
import math

import jax
import jax.numpy as jnp
from jax import lax
from jax.experimental import pallas as pl
from jax.experimental.pallas import tpu as pltpu
from jax.sharding import Mesh, PartitionSpec as P


TILE = 128
SLOTS = 32
W = 1024
NB = W // 128
CHUNK = 4
GROUP = 8
DEEP = 4
F32 = jnp.float32
BF16 = jnp.bfloat16
BLOCKS = [(i, j) for i in range(NB) for j in range(i, NB)]
HALF = len(BLOCKS) // 2
CHIPS = ("y", "z", "x")


def gram_kernel(heights_ref, a_ref, mine_ref, other_ref, acc_ref, buf_ref, sems):
    core = lax.axis_index("core")
    live = heights_ref[lax.axis_index("z") * lax.axis_size("x") + lax.axis_index("x")]
    count = lax.div(live + (CHUNK - 1), CHUNK)
    rows = CHUNK * TILE

    def load(at):
        slot = lax.rem(at, DEEP)
        first = pl.multiple_of(at * rows, rows)
        return pltpu.make_async_copy(a_ref.at[pl.ds(first, rows)], buf_ref.at[slot], sems.at[slot])

    for early in range(DEEP - 1):

        @pl.when(early < count)
        def _():
            load(early).start()

    acc_ref[...] = jnp.zeros_like(acc_ref)

    def accumulate(x):
        flipped = x.T
        for j in range(0, W, 256):
            acc_ref[: j + 256, j : j + 256] += jnp.dot(
                flipped[: j + 256], x[:, j : j + 256], preferred_element_type=F32
            )

    def chunk(at, carry):
        @pl.when(at + DEEP - 1 < count)
        def _():
            load(at + DEEP - 1).start()

        load(at).wait()
        here = buf_ref.at[lax.rem(at, DEEP)]

        @pl.when((at + 1) * CHUNK > live)
        def _():
            kept = lax.broadcasted_iota(jnp.int32, (rows, W), 0) < (live - at * CHUNK) * TILE
            here[...] = jnp.where(kept, here[...].astype(F32), 0.0).astype(BF16)

        accumulate(here[...])
        return carry

    lax.fori_loop(0, count, chunk, 0)

    def put(ref, blocks):
        for b, (i, j) in enumerate(blocks):
            ref[b] = acc_ref[i * 128 : i * 128 + 128, j * 128 : j * 128 + 128]

    @pl.when(core == 0)
    def _():
        put(mine_ref, BLOCKS[:HALF])
        put(other_ref, BLOCKS[HALF:])

    @pl.when(core == 1)
    def _():
        put(mine_ref, BLOCKS[HALF:])
        put(other_ref, BLOCKS[:HALF])


def gram(a_rows, heights):
    return pl.pallas_call(
        gram_kernel,
        in_specs=[pl.BlockSpec(memory_space=pltpu.SMEM), pl.BlockSpec(memory_space=pltpu.HBM)],
        out_specs=[pl.BlockSpec(memory_space=pltpu.VMEM)] * 2,
        scratch_shapes=[
            pltpu.VMEM((W, W), F32),
            pltpu.VMEM((DEEP, CHUNK * TILE, W), BF16),
            pltpu.SemaphoreType.DMA((DEEP,)),
        ],
        out_shape=[jax.ShapeDtypeStruct((HALF, 128, 128), F32)] * 2,
        compiler_params=pltpu.CompilerParams(vmem_limit_bytes=52 * 1024 * 1024),
        name="gram",
    )(heights, a_rows)


def pick_kernel(index_ref, a_ref, *refs):
    outs, (buf_ref, in_sems, out_sems) = refs[:-3], refs[-3:]
    count = len(outs)
    loads = [
        pltpu.make_async_copy(a_ref.at[pl.ds(pl.multiple_of(index_ref[i] * TILE, TILE), TILE)], buf_ref.at[i], in_sems.at[i])
        for i in range(count)
    ]
    stores = [pltpu.make_async_copy(buf_ref.at[i], outs[i], out_sems.at[i]) for i in range(count)]
    for load in loads:
        load.start()
    for load, store in zip(loads, stores):
        load.wait()
        store.start()
    for store in stores:
        store.wait()


def pick_tiles(a_rows, index):
    count = index.shape[0]
    return pl.pallas_call(
        pick_kernel,
        in_specs=[pl.BlockSpec(memory_space=pltpu.SMEM), pl.BlockSpec(memory_space=pltpu.HBM)],
        out_specs=[pl.BlockSpec(memory_space=pltpu.HBM)] * count,
        scratch_shapes=[
            pltpu.VMEM((count, TILE, W), BF16),
            pltpu.SemaphoreType.DMA((count,)),
            pltpu.SemaphoreType.DMA((count,)),
        ],
        out_shape=[jax.ShapeDtypeStruct((TILE, W), BF16)] * count,
        compiler_params=pltpu.CompilerParams(vmem_limit_bytes=56 * 1024 * 1024),
        name="pick",
    )(index, a_rows)


def lane_bcast(v, lane):
    return jnp.broadcast_to(v[:, lane : lane + 1], (8, 128))


def row_bcast(ref, p, s):
    return jnp.broadcast_to(ref[p, s : s + 1, :], (8, 128))


def factor_block(d_ref, rk_ref, dk_ref, es_ref, ms_ref, vs_ref):
    sub = lax.broadcasted_iota(jnp.int32, (8, 128), 0)
    lane = lax.broadcasted_iota(jnp.int32, (8, 128), 1)
    v = [d_ref[8 * g : 8 * g + 8, :] for g in range(16)]
    columns = [lane_bcast(v[0], j) for j in range(8)]
    for p in range(16):
        for j in range(8):
            es_ref[8 * p + j] = columns[j]
        vs_ref[p] = v[p]
        e = {(i, j): row_bcast(es_ref, 8 * p + j, i) for j in range(8) for i in range(j, 8)}
        inside = (lane >= 8 * p) & (lane < 8 * p + 8)
        low, inv, rows, wide, both = {}, [], [], [], []
        for s in range(8):
            inv.append(lax.rsqrt(e[s, s]))
            for i in range(s + 1, 8):
                low[i, s] = e[i, s] * inv[s]
            for j in range(s + 1, 8):
                for i in range(j, 8):
                    e[i, j] = e[i, j] - low[i, s] * low[j, s]
            r, q = row_bcast(vs_ref, p, s), jnp.where(lane == 8 * p + s, 1.0, 0.0).astype(F32)
            for t in range(s):
                r = r - low[s, t] * rows[t]
                q = q - low[s, t] * wide[t]
            rows.append(r * inv[s])
            wide.append(q * inv[s])
            both.append(jnp.where(inside, wide[s], rows[s]))
            rk_ref[8 * p + s : 8 * p + s + 1, :] = rows[s][0:1]
            dk_ref[8 * p + s : 8 * p + s + 1, :] = both[s][0:1]
        if p == 15:
            break
        after = 8 * p + 8
        columns = [lane_bcast(v[p + 1], after + j) for j in range(8)]
        for s in range(8):
            m = jnp.take_along_axis(rows[s], sub + after, axis=1, mode="promise_in_bounds")
            ms_ref[8 * p + s] = m
            for j in range(8):
                columns[j] = columns[j] - m * row_bcast(ms_ref, 8 * p + s, j)
        for g in range(p + 1, 16):
            v[g] = jnp.where(inside, 0.0, v[g])
            for s in range(8):
                m = jnp.take_along_axis(rows[s], sub + 8 * g, axis=1, mode="promise_in_bounds")
                v[g] = v[g] - m * both[s]


PASSES = 6
LEFT, RIGHT = ("mhh", "hmh") if PASSES == 3 else ("lhhmmh", "hlmhmh")


def split(x):
    h = x.astype(BF16)
    r = x - h.astype(F32)
    m = r.astype(BF16)
    return {"h": h, "m": m, "l": (r - m.astype(F32)).astype(BF16) if PASSES > 3 else None}


def put_left(ref, x):
    parts = split(x)
    for at, name in enumerate(LEFT):
        ref[:, at * 128 : at * 128 + 128] = parts[name]


def put_right(ref, x):
    parts = split(x)
    for at, name in enumerate(RIGHT):
        ref[at * 128 : at * 128 + 128] = parts[name]


def product(left_ref, right_ref):
    return jnp.dot(left_ref[...], right_ref[...], preferred_element_type=F32)


def chol_kernel(root, mine_ref, other_ref, hi_ref, lo_ref, r_ref, t_ref, d_ref, rk_ref, dk_ref, p_ref, left_ref, right_ref, es_ref, ms_ref, vs_ref, hi_out, lo_out, r_out, in_sems, out_sems):
    core = lax.axis_index("core")

    def block_copy(ref, b, at):
        i, j = BLOCKS[at]
        return pltpu.make_async_copy(
            ref.at[b], t_ref.at[i * 128 : i * 128 + 128, j * 128 : j * 128 + 128], in_sems.at[at]
        )

    for owner in range(2):

        @pl.when(core == owner)
        def _():
            for b in range(HALF):
                block_copy(mine_ref, b, owner * HALF + b).start()
            for b in range(HALF):
                block_copy(other_ref, b, (1 - owner) * HALF + b).start()

    def arrived(first, last):
        for at in range(first, last):
            block_copy(mine_ref, 0, at).wait()

    arrived(0, NB)
    sub = lax.broadcasted_iota(jnp.int32, (128, 128), 0)
    lane = lax.broadcasted_iota(jnp.int32, (128, 128), 1)
    wide_lane = lax.broadcasted_iota(jnp.int32, (128, W), 1)

    def leave(k):
        slot = lax.rem(k, 2)
        here = pl.ds(pl.multiple_of(k * 128, 128), 128)
        return [
            pltpu.make_async_copy(stage.at[slot], out.at[here], out_sems.at[n, slot])
            for n, (stage, out) in enumerate(((hi_out, hi_ref), (lo_out, lo_ref), (r_out, r_ref)))
        ]

    def block_row(k, carry):
        at = pl.multiple_of(k * 128, 128)
        here = pl.ds(at, 128)
        slot = lax.rem(k, 2)
        d_ref[...] = t_ref[here, here]
        factor_block(d_ref, rk_ref, dk_ref, es_ref, ms_ref, vs_ref)
        dk_ref[...] = jnp.where(lane <= sub, dk_ref[...], 0.0)
        put_left(left_ref.at[0:128], dk_ref[...])
        put_right(right_ref, t_ref[here, :])
        p_ref[...] = product(left_ref.at[0:128], right_ref)

        @pl.when(k >= 2)
        def _():
            for copy in leave(k - 2):
                copy.wait()

        r_out[slot] = jnp.where(wide_lane >= at + 128, p_ref[...] * (1.0 / root), 0.0)
        r_out[slot, :, here] = jnp.where(lane >= sub, rk_ref[...] * (1.0 / root), 0.0)
        p_ref[:, here] = dk_ref[...]
        scaled = jnp.where(wide_lane < at + 128, p_ref[...] * root, 0.0)
        hi = scaled.astype(BF16)
        hi_out[slot] = hi
        lo_out[slot] = (scaled - hi.astype(F32)).astype(BF16)
        for copy in leave(k):
            copy.start()

        @pl.when(k == 0)
        def _():
            arrived(NB, 2 * HALF)

        put_right(right_ref, p_ref[...])

        def trailing(first):
            put_left(left_ref.at[first:W], p_ref[:, first:].T)
            t_ref[first:, here] = jnp.zeros((W - first, 128), F32)
            for j in range(0, W, 256):
                t_ref[first:, j : j + 256] -= product(left_ref.at[first:W], right_ref.at[:, j : j + 256])

        for first in range(0, W, 256):
            pl.when((lax.div(k + 1, 2) * 256 == first) & (k < NB - 1))(lambda first=first: trailing(first))

        return carry

    lax.fori_loop(0, NB, block_row, 0)
    for k in (NB - 2, NB - 1):
        for copy in leave(k):
            copy.wait()


def cholesky(mine, other, root):
    hbm = pl.BlockSpec(memory_space=pltpu.HBM)
    return pl.pallas_call(
        lambda *refs: chol_kernel(root, *refs),
        out_shape=[
            jax.ShapeDtypeStruct((W, W), BF16),
            jax.ShapeDtypeStruct((W, W), BF16),
            jax.ShapeDtypeStruct((W, W), F32),
        ],
        in_specs=[hbm] * 2,
        out_specs=[hbm] * 3,
        scratch_shapes=[
            pltpu.VMEM((W, W), F32),
            pltpu.VMEM((128, 128), F32),
            pltpu.VMEM((128, 128), F32),
            pltpu.VMEM((128, 128), F32),
            pltpu.VMEM((128, W), F32),
            pltpu.VMEM((W, 128 * PASSES), BF16),
            pltpu.VMEM((128 * PASSES, W), BF16),
            pltpu.VMEM((128, 8, 128), F32),
            pltpu.VMEM((128, 8, 128), F32),
            pltpu.VMEM((16, 8, 128), F32),
            pltpu.VMEM((2, 128, W), BF16),
            pltpu.VMEM((2, 128, W), BF16),
            pltpu.VMEM((2, 128, W), F32),
            pltpu.SemaphoreType.DMA((2 * HALF,)),
            pltpu.SemaphoreType.DMA((3, 2)),
        ],
        cost_estimate=pl.CostEstimate(flops=40_000_000_000, bytes_accessed=16_000_000, transcendentals=0),
        compiler_params=pltpu.CompilerParams(vmem_limit_bytes=50 * 1024 * 1024),
        name="factor",
    )(mine, other)


def ortho_kernel(own_ref, arrive_ref, a_ref, hi_hbm, lo_hbm, *refs):
    came, (out_ref, buf_ref, hi_ref, lo_ref, sems, w_sems) = refs[:-6], refs[-6:]
    step = pl.program_id(0)

    def fetch(src, slot):
        return pltpu.make_async_copy(src, buf_ref.at[pl.ds(pl.multiple_of(slot * TILE, TILE), TILE)], sems.at[slot])

    def weights(j):
        part = (pl.ds(j, 256), pl.ds(0, j + 256))
        return [
            pltpu.make_async_copy(src.at[part], dst.at[part], w_sems.at[n, j // 256])
            for n, (src, dst) in enumerate(((hi_hbm, hi_ref), (lo_hbm, lo_ref)))
        ]

    @pl.when(step == 0)
    def _():
        for j in range(0, W, 256):
            for copy in weights(j):
                copy.start()

        def own(slot, carry):
            tile = own_ref[slot]

            @pl.when(tile >= 0)
            def _():
                fetch(a_ref.at[pl.ds(pl.multiple_of(tile * TILE, TILE), TILE)], slot).start()

            return carry

        lax.fori_loop(0, SLOTS, own, 0)
        for n, ref in enumerate(came):
            slot = arrive_ref[n]

            @pl.when(slot >= 0)
            def _():
                fetch(ref, slot).start()

    for g in range(GROUP):
        slot = step * GROUP + g
        full = own_ref[slot] >= 0
        for n in range(len(came)):
            full |= arrive_ref[n] == slot

        @pl.when(full)
        def _():
            fetch(a_ref.at[pl.ds(0, TILE)], slot).wait()

        @pl.when(jnp.logical_not(full))
        def _():
            buf_ref[pl.ds(pl.multiple_of(slot * TILE, TILE), TILE)] = jnp.zeros((TILE, W), BF16)

    @pl.when(step == 0)
    def _():
        for j in range(0, W, 256):
            for copy in weights(j):
                copy.wait()

    nt = (((1,), (1,)), ((), ()))
    rows = pl.ds(pl.multiple_of(step * (GROUP * TILE), GROUP * TILE), GROUP * TILE)
    for j in range(0, W, 256):
        x = buf_ref[rows, : j + 256]
        acc = lax.dot_general(x, hi_ref[j : j + 256, : j + 256], nt, preferred_element_type=F32)
        acc += lax.dot_general(x, lo_ref[j : j + 256, : j + 256], nt, preferred_element_type=F32)
        out_ref[:, j : j + 256] = acc.astype(BF16)


def ortho(a_rows, received, own, arrive, hi, lo):
    return pl.pallas_call(
        ortho_kernel,
        grid_spec=pltpu.PrefetchScalarGridSpec(
            num_scalar_prefetch=2,
            grid=(SLOTS // GROUP,),
            in_specs=[pl.BlockSpec(memory_space=pltpu.HBM)] * (3 + len(received)),
            out_specs=pl.BlockSpec((GROUP * TILE, W), lambda step, *_: (step, 0)),
            scratch_shapes=[
                pltpu.VMEM((SLOTS * TILE, W), BF16),
                pltpu.VMEM((W, W), BF16),
                pltpu.VMEM((W, W), BF16),
                pltpu.SemaphoreType.DMA((SLOTS,)),
                pltpu.SemaphoreType.DMA((2, W // 256)),
            ],
        ),
        out_shape=jax.ShapeDtypeStruct((SLOTS * TILE, W), BF16),
        compiler_params=pltpu.CompilerParams(vmem_limit_bytes=50 * 1024 * 1024),
        name="ortho",
    )(own, arrive, a_rows, hi, lo, *received)


def shift(pos, dz, dx):
    size_z, size_x = lax.axis_size("z"), lax.axis_size("x")
    return (pos // size_x + dz) % size_z * size_x + (pos % size_x + dx) % size_x


def shifts():
    pairs = [(dz, dx) for dz in range(lax.axis_size("z")) for dx in range(lax.axis_size("x"))]
    return pairs[1:]


def plan(heights, destination):
    size_gy = lax.axis_size("z") * lax.axis_size("x")
    group_pos = lax.axis_index("z") * lax.axis_size("x") + lax.axis_index("x")
    group_base = (lax.axis_index("y") * lax.axis_size("core") + lax.axis_index("core")) * size_gy
    my_index = group_base + group_pos
    tile_ids = jnp.arange(destination.shape[1], dtype=jnp.int32)
    peers = jnp.arange(size_gy, dtype=jnp.int32)
    slot_ids = jnp.arange(SLOTS, dtype=jnp.int32)
    moves = jnp.array(shifts(), jnp.int32)
    to = shift(group_pos, moves[:, 0], moves[:, 1])
    source = shift(group_pos, -moves[:, 0], -moves[:, 1])
    mine = peers == group_pos
    own_live = tile_ids < jnp.sum(jnp.where(mine, heights, 0))
    own_dest = jnp.sum(jnp.where(mine[:, None], destination, 0), axis=0)
    chosen = own_live[None, :] & ((own_dest // SLOTS)[None, :] == (group_base + to)[:, None])
    send_index = jnp.sum(jnp.where(chosen, tile_ids[None, :], 0), axis=1)
    landed = own_live[None, :] & (own_dest[None, :] == (my_index * SLOTS + slot_ids)[:, None])
    arriving = (tile_ids[None, :] < heights[:, None]) & (destination // SLOTS == my_index)
    by_peer = jnp.sum(jnp.where(arriving, destination % SLOTS + 1, 0), axis=1) - 1
    own = jnp.sum(jnp.where(landed, tile_ids[None, :] + 1, 0), axis=1) - 1
    arrive = jnp.sum(jnp.where(source[:, None] == peers[None, :], by_peer[None, :], 0), axis=1)
    return send_index, own, arrive


def swap_core(x):
    return lax.ppermute(x, "core", [(0, 1), (1, 0)])


def exchange(x, axes):
    return lax.all_to_all(x, axes, split_axis=0, concat_axis=0, tiled=True)


def on_device(a_rows, heights, destination):
    chips = math.prod(lax.axis_size(name) for name in CHIPS)
    root = math.sqrt(chips * 2 * SLOTS * TILE)
    mine, other = gram(a_rows, heights)
    half = (mine + swap_core(other)).reshape(chips, -1, 128)
    parts = exchange(half, CHIPS)
    send_index, own, arrive = plan(heights, destination)
    tiles = pick_tiles(a_rows, send_index)
    shard = jnp.sum(parts, axis=0)
    full = exchange(jnp.broadcast_to(shard[None], half.shape), CHIPS)
    size_gy = lax.axis_size("z") * lax.axis_size("x")
    received = [
        lax.ppermute(tile, ("z", "x"), [(i, shift(i, *move)) for i in range(size_gy)])
        for tile, move in zip(tiles, shifts())
    ]
    mine = full.reshape(HALF, 128, 128)
    other = swap_core(mine)
    hi, lo, factor_r = cholesky(mine, other, root)
    ortho_rows = ortho(a_rows, received, own, arrive, hi, lo)
    return (ortho_rows, factor_r)


def solution(mesh):
    fine = Mesh(mesh.devices.reshape(4, 2, 4, 4), ("y", "core", "z", "x"))
    every = ("y", "core", "z", "x")
    return jax.shard_map(
        on_device,
        mesh=fine,
        in_specs=(P(every, None), P(("y", "core")), P(("y", "core"), None)),
        out_specs=(P(every, None), P()),
        check_vma=False,
    )
```

```python
import math

import jax
import jax.numpy as jnp
from jax import lax
from jax.experimental import pallas as pl
from jax.experimental.pallas import tpu as pltpu
from jax.sharding import Mesh, PartitionSpec as P


TILE = 128
SLOTS = 32
W = 1024
NB = W // 128
CHUNK = 4
GROUP = 8
DEEP = 4
F32 = jnp.float32
BF16 = jnp.bfloat16
BLOCKS = [(i, j) for i in range(NB) for j in range(i, NB)]
HALF = len(BLOCKS) // 2
ROOM = 20
CHIPS = ("y", "z", "x")


def gram_kernel(heights_ref, a_ref, mine_ref, other_ref, acc_ref, buf_ref, sems):
    core = lax.axis_index("core")
    live = heights_ref[lax.axis_index("z") * lax.axis_size("x") + lax.axis_index("x")]
    count = lax.div(live + (CHUNK - 1), CHUNK)
    rows = CHUNK * TILE

    def load(at):
        slot = lax.rem(at, DEEP)
        first = pl.multiple_of(at * rows, rows)
        return pltpu.make_async_copy(a_ref.at[pl.ds(first, rows)], buf_ref.at[slot], sems.at[slot])

    for early in range(DEEP - 1):

        @pl.when(early < count)
        def _():
            load(early).start()

    acc_ref[...] = jnp.zeros_like(acc_ref)

    def accumulate(x):
        flipped = x.T
        for j in range(0, W, 256):
            acc_ref[: j + 256, j : j + 256] += jnp.dot(
                flipped[: j + 256], x[:, j : j + 256], preferred_element_type=F32
            )

    def chunk(at, carry):
        @pl.when(at + DEEP - 1 < count)
        def _():
            load(at + DEEP - 1).start()

        load(at).wait()
        here = buf_ref.at[lax.rem(at, DEEP)]

        @pl.when((at + 1) * CHUNK > live)
        def _():
            kept = lax.broadcasted_iota(jnp.int32, (rows, W), 0) < (live - at * CHUNK) * TILE
            here[...] = jnp.where(kept, here[...].astype(F32), 0.0).astype(BF16)

        accumulate(here[...])
        return carry

    lax.fori_loop(0, count, chunk, 0)

    def put(ref, blocks):
        for b, (i, j) in enumerate(blocks):
            ref[b] = acc_ref[i * 128 : i * 128 + 128, j * 128 : j * 128 + 128]

    for ref in (mine_ref, other_ref):
        ref[HALF:] = jnp.zeros((ROOM - HALF, 128, 128), F32)

    @pl.when(core == 0)
    def _():
        put(mine_ref, BLOCKS[:HALF])
        put(other_ref, BLOCKS[HALF:])

    @pl.when(core == 1)
    def _():
        put(mine_ref, BLOCKS[HALF:])
        put(other_ref, BLOCKS[:HALF])


def gram(a_rows, heights):
    return pl.pallas_call(
        gram_kernel,
        in_specs=[pl.BlockSpec(memory_space=pltpu.SMEM), pl.BlockSpec(memory_space=pltpu.HBM)],
        out_specs=[pl.BlockSpec(memory_space=pltpu.VMEM)] * 2,
        scratch_shapes=[
            pltpu.VMEM((W, W), F32),
            pltpu.VMEM((DEEP, CHUNK * TILE, W), BF16),
            pltpu.SemaphoreType.DMA((DEEP,)),
        ],
        out_shape=[jax.ShapeDtypeStruct((ROOM, 128, 128), F32)] * 2,
        compiler_params=pltpu.CompilerParams(vmem_limit_bytes=52 * 1024 * 1024),
        name="gram",
    )(heights, a_rows)


def pick_kernel(index_ref, a_ref, *refs):
    outs, (buf_ref, in_sems, out_sems) = refs[:-3], refs[-3:]
    count = len(outs)
    loads = [
        pltpu.make_async_copy(a_ref.at[pl.ds(pl.multiple_of(index_ref[i] * TILE, TILE), TILE)], buf_ref.at[i], in_sems.at[i])
        for i in range(count)
    ]
    stores = [pltpu.make_async_copy(buf_ref.at[i], outs[i], out_sems.at[i]) for i in range(count)]
    for load in loads:
        load.start()
    for load, store in zip(loads, stores):
        load.wait()
        store.start()
    for store in stores:
        store.wait()


def pick_tiles(a_rows, index):
    count = index.shape[0]
    return pl.pallas_call(
        pick_kernel,
        in_specs=[pl.BlockSpec(memory_space=pltpu.SMEM), pl.BlockSpec(memory_space=pltpu.HBM)],
        out_specs=[pl.BlockSpec(memory_space=pltpu.HBM)] * count,
        scratch_shapes=[
            pltpu.VMEM((count, TILE, W), BF16),
            pltpu.SemaphoreType.DMA((count,)),
            pltpu.SemaphoreType.DMA((count,)),
        ],
        out_shape=[jax.ShapeDtypeStruct((TILE, W), BF16)] * count,
        compiler_params=pltpu.CompilerParams(vmem_limit_bytes=56 * 1024 * 1024),
        name="pick",
    )(index, a_rows)


def lane_bcast(v, lane):
    return jnp.broadcast_to(v[:, lane : lane + 1], (8, 128))


def row_bcast(ref, p, s):
    return jnp.broadcast_to(ref[p, s : s + 1, :], (8, 128))


def factor_block(d_ref, rk_ref, dk_ref, es_ref, ms_ref, vs_ref):
    sub = lax.broadcasted_iota(jnp.int32, (8, 128), 0)
    lane = lax.broadcasted_iota(jnp.int32, (8, 128), 1)
    v = [d_ref[8 * g : 8 * g + 8, :] for g in range(16)]
    columns = [lane_bcast(v[0], j) for j in range(8)]
    for p in range(16):
        for j in range(8):
            es_ref[8 * p + j] = columns[j]
        vs_ref[p] = v[p]
        e = {(i, j): row_bcast(es_ref, 8 * p + j, i) for j in range(8) for i in range(j, 8)}
        inside = (lane >= 8 * p) & (lane < 8 * p + 8)
        low, inv, rows, wide, both = {}, [], [], [], []
        for s in range(8):
            inv.append(lax.rsqrt(e[s, s]))
            for i in range(s + 1, 8):
                low[i, s] = e[i, s] * inv[s]
            for j in range(s + 1, 8):
                for i in range(j, 8):
                    e[i, j] = e[i, j] - low[i, s] * low[j, s]
            r, q = row_bcast(vs_ref, p, s), jnp.where(lane == 8 * p + s, 1.0, 0.0).astype(F32)
            for t in range(s):
                r = r - low[s, t] * rows[t]
                q = q - low[s, t] * wide[t]
            rows.append(r * inv[s])
            wide.append(q * inv[s])
            both.append(jnp.where(inside, wide[s], rows[s]))
            rk_ref[8 * p + s : 8 * p + s + 1, :] = rows[s][0:1]
            dk_ref[8 * p + s : 8 * p + s + 1, :] = both[s][0:1]
        if p == 15:
            break
        after = 8 * p + 8
        columns = [lane_bcast(v[p + 1], after + j) for j in range(8)]
        for s in range(8):
            m = jnp.take_along_axis(rows[s], sub + after, axis=1, mode="promise_in_bounds")
            ms_ref[8 * p + s] = m
            for j in range(8):
                columns[j] = columns[j] - m * row_bcast(ms_ref, 8 * p + s, j)
        for g in range(p + 1, 16):
            v[g] = jnp.where(inside, 0.0, v[g])
            for s in range(8):
                m = jnp.take_along_axis(rows[s], sub + 8 * g, axis=1, mode="promise_in_bounds")
                v[g] = v[g] - m * both[s]


PASSES = 6
LEFT, RIGHT = ("mhh", "hmh") if PASSES == 3 else ("lhhmmh", "hlmhmh")


def split(x):
    h = x.astype(BF16)
    r = x - h.astype(F32)
    m = r.astype(BF16)
    return {"h": h, "m": m, "l": (r - m.astype(F32)).astype(BF16) if PASSES > 3 else None}


def put_left(ref, x):
    parts = split(x)
    for at, name in enumerate(LEFT):
        ref[:, at * 128 : at * 128 + 128] = parts[name]


def put_right(ref, x):
    parts = split(x)
    for at, name in enumerate(RIGHT):
        ref[at * 128 : at * 128 + 128] = parts[name]


def product(left_ref, right_ref):
    return jnp.dot(left_ref[...], right_ref[...], preferred_element_type=F32)


def chol_kernel(root, mine_ref, other_ref, hi_ref, lo_ref, r_ref, t_ref, d_ref, rk_ref, dk_ref, p_ref, row_ref, small_ref, left_ref, right_ref, es_ref, ms_ref, vs_ref, hi_out, lo_out, r_out, in_sems, out_sems):
    core = lax.axis_index("core")

    def block_copy(ref, b, at):
        i, j = BLOCKS[at]
        return pltpu.make_async_copy(
            ref.at[b], t_ref.at[i * 128 : i * 128 + 128, j * 128 : j * 128 + 128], in_sems.at[at]
        )

    for owner in range(2):

        @pl.when(core == owner)
        def _():
            for b in range(HALF):
                block_copy(mine_ref, b, owner * HALF + b).start()
            for b in range(HALF):
                block_copy(other_ref, b, (1 - owner) * HALF + b).start()

    def arrived(first, last):
        for at in range(first, last):
            block_copy(mine_ref, 0, at).wait()

    arrived(0, 2 * HALF)
    sub = lax.broadcasted_iota(jnp.int32, (128, 128), 0)
    lane = lax.broadcasted_iota(jnp.int32, (128, 128), 1)
    wide_lane = lax.broadcasted_iota(jnp.int32, (128, W), 1)

    def leave(k):
        slot = lax.rem(k, 2)
        here = pl.ds(pl.multiple_of(k * 128, 128), 128)
        return [
            pltpu.make_async_copy(stage.at[slot], out.at[here], out_sems.at[n, slot])
            for n, (stage, out) in enumerate(((hi_out, hi_ref), (lo_out, lo_ref), (r_out, r_ref)))
        ]

    left_ref[...] = jnp.zeros_like(left_ref)
    right_ref[...] = jnp.zeros_like(right_ref)
    row_ref[...] = t_ref[0:128, :]

    def block_row(k, carry):
        at = pl.multiple_of(k * 128, 128)
        here = pl.ds(at, 128)
        slot = lax.rem(k, 2)
        d_ref[...] = row_ref[:, here]

        factor_block(d_ref, rk_ref, dk_ref, es_ref, ms_ref, vs_ref)
        for j in range(0, W, 256):
            t_ref[:, j : j + 256] -= product(left_ref, right_ref.at[:, j : j + 256])
        dk_ref[...] = jnp.where(lane <= sub, dk_ref[...], 0.0)
        put_left(small_ref, dk_ref[...])
        put_right(right_ref, row_ref[...])
        p_ref[...] = product(small_ref, right_ref)

        @pl.when(k >= 2)
        def _():
            for copy in leave(k - 2):
                copy.wait()

        r_out[slot] = jnp.where(wide_lane >= at + 128, p_ref[...] * (1.0 / root), 0.0)
        r_out[slot, :, here] = jnp.where(lane >= sub, rk_ref[...] * (1.0 / root), 0.0)
        p_ref[:, here] = dk_ref[...]
        scaled = jnp.where(wide_lane < at + 128, p_ref[...] * root, 0.0)
        hi = scaled.astype(BF16)
        hi_out[slot] = hi
        lo_out[slot] = (scaled - hi.astype(F32)).astype(BF16)
        for copy in leave(k):
            copy.start()

        @pl.when(k < NB - 1)
        def _():
            below = pl.ds(pl.multiple_of(at + 128, 128), 128)
            put_right(right_ref, p_ref[...])
            put_left(left_ref, p_ref[...].T)
            t_ref[:, here] = jnp.zeros((W, 128), F32)
            row_ref[...] = t_ref[below, :] - product(left_ref.at[below], right_ref)

        return carry

    lax.fori_loop(0, NB, block_row, 0)
    for k in (NB - 2, NB - 1):
        for copy in leave(k):
            copy.wait()


def cholesky(mine, other, root):
    hbm = pl.BlockSpec(memory_space=pltpu.HBM)
    return pl.pallas_call(
        lambda *refs: chol_kernel(root, *refs),
        out_shape=[
            jax.ShapeDtypeStruct((W, W), BF16),
            jax.ShapeDtypeStruct((W, W), BF16),
            jax.ShapeDtypeStruct((W, W), F32),
        ],
        in_specs=[hbm] * 2,
        out_specs=[hbm] * 3,
        scratch_shapes=[
            pltpu.VMEM((W, W), F32),
            pltpu.VMEM((128, 128), F32),
            pltpu.VMEM((128, 128), F32),
            pltpu.VMEM((128, 128), F32),
            pltpu.VMEM((128, W), F32),
            pltpu.VMEM((128, W), F32),
            pltpu.VMEM((128, 128 * PASSES), BF16),
            pltpu.VMEM((W, 128 * PASSES), BF16),
            pltpu.VMEM((128 * PASSES, W), BF16),
            pltpu.VMEM((128, 8, 128), F32),
            pltpu.VMEM((128, 8, 128), F32),
            pltpu.VMEM((16, 8, 128), F32),
            pltpu.VMEM((2, 128, W), BF16),
            pltpu.VMEM((2, 128, W), BF16),
            pltpu.VMEM((2, 128, W), F32),
            pltpu.SemaphoreType.DMA((2 * HALF,)),
            pltpu.SemaphoreType.DMA((3, 2)),
        ],
        cost_estimate=pl.CostEstimate(flops=40_000_000_000, bytes_accessed=16_000_000, transcendentals=0),
        compiler_params=pltpu.CompilerParams(vmem_limit_bytes=50 * 1024 * 1024),
        name="factor",
    )(mine, other)


def ortho_kernel(own_ref, arrive_ref, a_ref, hi_hbm, lo_hbm, *refs):
    came, (out_ref, buf_ref, hi_ref, lo_ref, sems, w_sems) = refs[:-6], refs[-6:]
    step = pl.program_id(0)

    def fetch(src, slot):
        return pltpu.make_async_copy(src, buf_ref.at[pl.ds(pl.multiple_of(slot * TILE, TILE), TILE)], sems.at[slot])

    def weights(j):
        part = (pl.ds(j, 256), pl.ds(0, j + 256))
        return [
            pltpu.make_async_copy(src.at[part], dst.at[part], w_sems.at[n, j // 256])
            for n, (src, dst) in enumerate(((hi_hbm, hi_ref), (lo_hbm, lo_ref)))
        ]

    @pl.when(step == 0)
    def _():
        for j in range(0, W, 256):
            for copy in weights(j):
                copy.start()

        def own(slot, carry):
            tile = own_ref[slot]

            @pl.when(tile >= 0)
            def _():
                fetch(a_ref.at[pl.ds(pl.multiple_of(tile * TILE, TILE), TILE)], slot).start()

            return carry

        lax.fori_loop(0, SLOTS, own, 0)
        for n, ref in enumerate(came):
            slot = arrive_ref[n]

            @pl.when(slot >= 0)
            def _():
                fetch(ref, slot).start()

    for g in range(GROUP):
        slot = step * GROUP + g
        full = own_ref[slot] >= 0
        for n in range(len(came)):
            full |= arrive_ref[n] == slot

        @pl.when(full)
        def _():
            fetch(a_ref.at[pl.ds(0, TILE)], slot).wait()

        @pl.when(jnp.logical_not(full))
        def _():
            buf_ref[pl.ds(pl.multiple_of(slot * TILE, TILE), TILE)] = jnp.zeros((TILE, W), BF16)

    @pl.when(step == 0)
    def _():
        for j in range(0, W, 256):
            for copy in weights(j):
                copy.wait()

    nt = (((1,), (1,)), ((), ()))
    rows = pl.ds(pl.multiple_of(step * (GROUP * TILE), GROUP * TILE), GROUP * TILE)
    for j in range(0, W, 256):
        x = buf_ref[rows, : j + 256]
        acc = lax.dot_general(x, hi_ref[j : j + 256, : j + 256], nt, preferred_element_type=F32)
        acc += lax.dot_general(x, lo_ref[j : j + 256, : j + 256], nt, preferred_element_type=F32)
        out_ref[:, j : j + 256] = acc.astype(BF16)


def ortho(a_rows, received, own, arrive, hi, lo):
    return pl.pallas_call(
        ortho_kernel,
        grid_spec=pltpu.PrefetchScalarGridSpec(
            num_scalar_prefetch=2,
            grid=(SLOTS // GROUP,),
            in_specs=[pl.BlockSpec(memory_space=pltpu.HBM)] * (3 + len(received)),
            out_specs=pl.BlockSpec((GROUP * TILE, W), lambda step, *_: (step, 0)),
            scratch_shapes=[
                pltpu.VMEM((SLOTS * TILE, W), BF16),
                pltpu.VMEM((W, W), BF16),
                pltpu.VMEM((W, W), BF16),
                pltpu.SemaphoreType.DMA((SLOTS,)),
                pltpu.SemaphoreType.DMA((2, W // 256)),
            ],
        ),
        out_shape=jax.ShapeDtypeStruct((SLOTS * TILE, W), BF16),
        compiler_params=pltpu.CompilerParams(vmem_limit_bytes=50 * 1024 * 1024),
        name="ortho",
    )(own, arrive, a_rows, hi, lo, *received)


def shift(pos, dz, dx):
    size_z, size_x = lax.axis_size("z"), lax.axis_size("x")
    return (pos // size_x + dz) % size_z * size_x + (pos % size_x + dx) % size_x


def shifts():
    pairs = [(dz, dx) for dz in range(lax.axis_size("z")) for dx in range(lax.axis_size("x"))]
    return pairs[1:]


def plan(heights, destination):
    size_gy = lax.axis_size("z") * lax.axis_size("x")
    group_pos = lax.axis_index("z") * lax.axis_size("x") + lax.axis_index("x")
    group_base = (lax.axis_index("y") * lax.axis_size("core") + lax.axis_index("core")) * size_gy
    my_index = group_base + group_pos
    tile_ids = jnp.arange(destination.shape[1], dtype=jnp.int32)
    peers = jnp.arange(size_gy, dtype=jnp.int32)
    slot_ids = jnp.arange(SLOTS, dtype=jnp.int32)
    moves = jnp.array(shifts(), jnp.int32)
    to = shift(group_pos, moves[:, 0], moves[:, 1])
    source = shift(group_pos, -moves[:, 0], -moves[:, 1])
    mine = peers == group_pos
    own_live = tile_ids < jnp.sum(jnp.where(mine, heights, 0))
    own_dest = jnp.sum(jnp.where(mine[:, None], destination, 0), axis=0)
    chosen = own_live[None, :] & ((own_dest // SLOTS)[None, :] == (group_base + to)[:, None])
    send_index = jnp.sum(jnp.where(chosen, tile_ids[None, :], 0), axis=1)
    landed = own_live[None, :] & (own_dest[None, :] == (my_index * SLOTS + slot_ids)[:, None])
    arriving = (tile_ids[None, :] < heights[:, None]) & (destination // SLOTS == my_index)
    by_peer = jnp.sum(jnp.where(arriving, destination % SLOTS + 1, 0), axis=1) - 1
    own = jnp.sum(jnp.where(landed, tile_ids[None, :] + 1, 0), axis=1) - 1
    arrive = jnp.sum(jnp.where(source[:, None] == peers[None, :], by_peer[None, :], 0), axis=1)
    return send_index, own, arrive


def swap_core(x):
    return lax.ppermute(x, "core", [(0, 1), (1, 0)])


def exchange(x, axes):
    return lax.all_to_all(x, axes, split_axis=0, concat_axis=0, tiled=True)


def on_device(a_rows, heights, destination):
    chips = math.prod(lax.axis_size(name) for name in CHIPS)
    root = math.sqrt(chips * 2 * SLOTS * TILE)
    mine, other = gram(a_rows, heights)
    half = (mine + swap_core(other)).reshape(chips, -1, 128)
    parts = exchange(half, CHIPS)
    send_index, own, arrive = plan(heights, destination)
    tiles = pick_tiles(a_rows, send_index)
    shard = jnp.sum(parts, axis=0)
    full = exchange(jnp.broadcast_to(shard[None], half.shape), CHIPS)
    size_gy = lax.axis_size("z") * lax.axis_size("x")
    received = []
    for tile, move in zip(tiles, shifts()):
        received.append(lax.ppermute(tile, ("z", "x"), [(i, shift(i, *move)) for i in range(size_gy)]))
    mine = full.reshape(ROOM, 128, 128)
    other = swap_core(mine)
    hi, lo, factor_r = cholesky(mine, other, root)
    ortho_rows = ortho(a_rows, received, own, arrive, hi, lo)
    return (ortho_rows, factor_r)


def solution(mesh):
    fine = Mesh(mesh.devices.reshape(4, 2, 4, 4), ("y", "core", "z", "x"))
    every = ("y", "core", "z", "x")
    return jax.shard_map(
        on_device,
        mesh=fine,
        in_specs=(P(every, None), P(("y", "core")), P(("y", "core"), None)),
        out_specs=(P(every, None), P()),
        check_vma=False,
    )
```
